32 devices in a mesh: grp: 2 (over y), src: 4 (over z), snk: 4 (over x, core).
Axes of the slice: x: 2, y: 2, z: 4, core: 2. Of those that a mesh axis runs over, the one named last changes fastest.
Arguments:
- solutions: bfloat16 [8, 4, 2, 4, 64, 3, 128], P(('grp', 'src'), None, None, None, 'snk'), parts along dimension 0, may hold values from -6 to 6
- eigvecs: bfloat16 [8, 2, 64, 3, 512], P(('grp', 'snk')), parts along dimension 0, may hold values from -0.3125 to 0.3125
- momenta: int32 [8, 3], replicated, may hold values from -2 to 2
- ordering: int32 [512], replicated, may hold values from 0 to 511, each once
Outputs:
- peramb: bfloat16 [8, 4, 2, 512, 4, 128], P(('grp', 'snk'), 'src'), parts along dimension 0
- correlator: float32 [8, 4, 2, 8], P(('grp', 'snk'), 'src'), parts along dimension 0
The draws below stay inside these ranges and needn't reach their ends.
There are 2 independent parts, one for each index of `grp`. The reference program is written for one: setup_inputs(seed, part) draws one part's arguments, and reference() takes and returns one part's arrays. A program takes and returns all parts, laid end to end along the dimension named above; an argument that names none is the same for every part. Nothing has to cross between parts.
Inputs may be any that keep to these rules, and one draw needn't show every extreme that they name: `momenta`: components in units of 2 pi / 64; the third (z) has no effect on the window. `ordering`: each eigenvector index once.
All inputs are finite; a program needn't handle non-finite values.
Results may differ from the reference program's by a relative error of at most 0.0034.
Values may be sent and summed in bfloat16 or wider, within the bound.
No kernel may reach another device: no remote copies, remote signals or barrier semaphores. Data moves between devices by JAX's collectives and lax.ppermute only.
A program may use at most 64 MiB of HBM per device.

```python
import math
import jax
import jax.numpy as jnp
from jax import lax

NEV = 512
DILUTION_COUNT = 128
WINDOW_SITES = 64
LAT = 64
MOMS = 8
NB = 32
SOURCE_TIMES = 4
SINK_TIMES = 4


def with_ends(values, stream_key, smallest, largest):
    shape = values.shape
    spot = [jax.random.randint(jax.random.fold_in(stream_key, axis), (), 0, shape[axis]) for axis in range(len(shape))]
    values = values.at[tuple(spot)].set(smallest)
    longest = shape.index(max(shape))
    spot[longest] = (spot[longest] + 1) % shape[longest]
    return values.at[tuple(spot)].set(largest)


def steps_of(rng, dims, cuts, low, largest):
    def one(axis_at, shards_of):
        steps = jax.random.uniform(jax.random.fold_in(jax.random.fold_in(rng, 6), axis_at), (shards_of,), jnp.float32, low / len(cuts), largest / len(cuts))
        return jnp.repeat(jnp.exp(steps), dims[axis_at] // shards_of).reshape((-1,) + (1,) * (len(dims) - axis_at - 1))

    level = one(*cuts[0])
    for cut in cuts[1:]:
        level = level * one(*cut)
    return level


def noise(rng, extent, scale, reach, pieces=(), kind=jnp.bfloat16):
    result = jax.random.normal(rng, extent, jnp.float32) * scale
    if len(pieces) > 0:
        result = steps_of(rng, extent, pieces, -0.22, 0.18) * result
    return jnp.clip(result, min=-reach, max=reach).astype(kind)


def setup_inputs(seed: int = 0, part: int = 0) -> dict:
    keys = jax.random.split(jax.random.key(seed), 5)
    own_keys = jax.random.split(jax.random.fold_in(keys[4], part), 5)
    solutions = noise(own_keys[0], (SOURCE_TIMES, SINK_TIMES, 2, 4, WINDOW_SITES, 3, DILUTION_COUNT), 1.0, 6.0, ((0, 4), (4, 4)))
    eigvecs = noise(own_keys[1], (SINK_TIMES, 2, WINDOW_SITES, 3, NEV), (6 * WINDOW_SITES) ** -0.5, 0.3125, ((0, 4),))
    momenta = with_ends(jax.random.randint(keys[2], (MOMS, 3), -2, 3), jax.random.fold_in(keys[2], 1), -2, 2).astype(jnp.int32)
    ordering = jax.random.permutation(keys[3], NEV).astype(jnp.int32)
    return dict(solutions=solutions, eigvecs=eigvecs, momenta=momenta, ordering=ordering)


PRECISE = lax.Precision.HIGHEST
SPIN_SIGNS = (1.0, 1.0, -1.0, -1.0)


def einsum_full(form, *operands):
    return jnp.einsum(form, *[item.astype(jnp.float32) for item in operands], precision=PRECISE)


def phase_tables(momenta):
    lattice_site_index = jnp.arange(WINDOW_SITES, dtype=jnp.int32)
    coord_x = (lattice_site_index % LAT).astype(jnp.float32)
    coord_y = ((lattice_site_index // LAT) % LAT).astype(jnp.float32)
    coord_z = (lattice_site_index // (LAT * LAT)).astype(jnp.float32)
    momentum_f = momenta.astype(jnp.float32)
    phase_angle = (2.0 * math.pi / LAT) * (momentum_f[:, 0:1] * coord_x[None, :] + momentum_f[:, 1:2] * coord_y[None, :] + momentum_f[:, 2:3] * coord_z[None, :])
    return jnp.cos(phase_angle), jnp.sin(phase_angle)


def block_onehot(ordering):
    block_ids = jnp.arange(NB, dtype=jnp.int32)
    return (ordering[:, None] // (NEV // NB) == block_ids[None, :]).astype(jnp.bfloat16)


def elementals_from(factors, phase_cos, phase_sine_part):
    fac_real, fac_imag = factors[0], factors[1]
    pair_real = einsum_full('xce,xcb->xeb', fac_real, fac_real) + einsum_full('xce,xcb->xeb', fac_imag, fac_imag)
    pairing_imaginary = einsum_full('xce,xcb->xeb', fac_real, fac_imag) - einsum_full('xce,xcb->xeb', fac_imag, fac_real)
    elemental_real = einsum_full('px,xeb->peb', phase_cos, pair_real) + einsum_full('px,xeb->peb', phase_sine_part, pairing_imaginary)
    elem_imag = einsum_full('px,xeb->peb', phase_cos, pairing_imaginary) - einsum_full('px,xeb->peb', phase_sine_part, pair_real)
    return jnp.stack([elemental_real, elem_imag])


def source_elementals(eigen, onehot, phase_cos, phase_sine_part):
    factors = einsum_full('rxck,kb->rxcb', eigen, onehot)
    return elementals_from(factors, phase_cos, phase_sine_part)


def sink_side(eigen, solution, phase_cos, phase_sine_part, elementals):
    eig_real, eig_imag = eigen[0], eigen[1]
    sol_real, sol_imag = solution[0], solution[1]
    tau_real = einsum_full('xck,axcd->kad', eig_real, sol_real) + einsum_full('xck,axcd->kad', eig_imag, sol_imag)
    tau_imag = einsum_full('xck,axcd->kad', eig_real, sol_imag) - einsum_full('xck,axcd->kad', eig_imag, sol_real)
    peramb = jnp.stack([tau_real, tau_imag]).astype(jnp.bfloat16)
    smear_real = einsum_full('xck,kad->axcd', eig_real, peramb[0]) - einsum_full('xck,kad->axcd', eig_imag, peramb[1])
    smear_imag = einsum_full('xck,kad->axcd', eig_real, peramb[1]) + einsum_full('xck,kad->axcd', eig_imag, peramb[0])
    smear_real = smear_real.reshape(4, WINDOW_SITES, 3, 4, NB)
    smear_imag = smear_imag.reshape(4, WINDOW_SITES, 3, 4, NB)
    spin_sign = jnp.array(SPIN_SIGNS, dtype=jnp.float32)
    loop_real = einsum_full('a,axcsb,axcse->xbe', spin_sign, smear_real, smear_real) + einsum_full('a,axcsb,axcse->xbe', spin_sign, smear_imag, smear_imag)
    loop_imag = einsum_full('a,axcsb,axcse->xbe', spin_sign, smear_real, smear_imag) - einsum_full('a,axcsb,axcse->xbe', spin_sign, smear_imag, smear_real)
    sink_real = einsum_full('px,xbe->pbe', phase_cos, loop_real) - einsum_full('px,xbe->pbe', phase_sine_part, loop_imag)
    sink_imag = einsum_full('px,xbe->pbe', phase_cos, loop_imag) + einsum_full('px,xbe->pbe', phase_sine_part, loop_real)
    src_real, src_imag = elementals[0], elementals[1]
    corr_real = einsum_full('pbe,peb->p', sink_real, src_real) - einsum_full('pbe,peb->p', sink_imag, src_imag)
    corr_imag = einsum_full('pbe,peb->p', sink_real, src_imag) + einsum_full('pbe,peb->p', sink_imag, src_real)
    return peramb, jnp.stack([corr_real, corr_imag]) * (1.0 / (WINDOW_SITES * NB))


def reference(solutions, eigvecs, momenta, ordering):
    phase_cos, phase_sine_part = phase_tables(momenta)
    onehot = block_onehot(ordering)
    all_elementals = lax.map(lambda eigen: source_elementals(eigen, onehot, phase_cos, phase_sine_part), eigvecs)

    def per_sink(sink_time):
        eigen = eigvecs[sink_time]

        def per_source(source_time):
            return sink_side(eigen, solutions[source_time, sink_time], phase_cos, phase_sine_part, all_elementals[source_time])

        return lax.map(per_source, jnp.arange(SOURCE_TIMES, dtype=jnp.int32))

    peramb, correlator = lax.map(per_sink, jnp.arange(SINK_TIMES, dtype=jnp.int32))
    return peramb, correlator
```

```python
import functools
import math

import jax
import jax.numpy as jnp
from jax import lax
from jax.experimental import pallas as pl
from jax.experimental.pallas import tpu as pltpu
from jax.sharding import PartitionSpec as P

LAT = 64
SPIN_SIGNS = (1.0, 1.0, -1.0, -1.0)
F32, BF16 = jnp.float32, jnp.bfloat16
VMEM = pl.BlockSpec(memory_space=pltpu.VMEM)
SMEM = pl.BlockSpec(memory_space=pltpu.SMEM)
ANY = pl.BlockSpec(memory_space=pl.ANY)


def params(mib):
    return pltpu.CompilerParams(vmem_limit_bytes=mib << 20)


def factors_kernel(ord_ref, e_ref, hi_ref, lo_ref):
    nb = hi_ref.shape[0]
    parts, colours, sites, nev = e_ref.shape
    onehot = lax.broadcasted_iota(jnp.int32, (nb, nev), 0) == ord_ref[...] // (nev // nb)
    onehot = jnp.where(onehot, 1.0, 0.0).astype(BF16)
    fac = lax.dot_general(
        onehot, e_ref[...].reshape(parts * colours * sites, nev), (((1,), (1,)), ((), ())), preferred_element_type=F32
    )
    hi = fac.astype(BF16)
    hi_ref[...] = hi
    lo_ref[...] = (fac - hi.astype(F32)).astype(BF16)


def prepare_kernel(counts, mom_ref, e_ref, g_ref, et_ref, ee_ref, ct_ref):
    slots, share = counts
    _, colours, sites, nev = e_ref.shape
    half = colours * sites
    if g_ref is None:
        me = lax.axis_index("snk")
        first, second = [], []
        for j in range(slots):
            at = pl.ds(pl.multiple_of((me ^ j) * share, share), share)
            re = e_ref[0, :, at, :].reshape(colours * share, nev)
            im = e_ref[1, :, at, :].reshape(colours * share, nev)
            first += [re, im]
            second += [-im, re]
    else:
        first, second = [g_ref[0], g_ref[1]], [-g_ref[1], g_ref[0]]
    et_ref[:nev, :] = jnp.concatenate(first, axis=0).T
    et_ref[nev:, :] = jnp.concatenate(second, axis=0).T
    re, im = e_ref[0].reshape(half, nev), e_ref[1].reshape(half, nev)
    ee_ref[:half, :nev] = re
    ee_ref[:half, nev:] = -im
    ee_ref[half:, :nev] = im
    ee_ref[half:, nev:] = re
    moms = ct_ref.shape[0] // 2
    row = lax.broadcasted_iota(jnp.int32, (sites, 2 * sites), 0)
    col = lax.broadcasted_iota(jnp.int32, (sites, 2 * sites), 1)
    col = jnp.where(col >= sites, col - sites, col)
    dx = row % LAT - col % LAT
    dy = row // LAT % LAT - col // LAT % LAT
    dz = row // (LAT * LAT) - col // (LAT * LAT)
    for p in range(moms):
        turn = mom_ref[p, 0] * dx + mom_ref[p, 1] * dy + mom_ref[p, 2] * dz
        angle = (2.0 * math.pi / LAT) * (turn & (LAT - 1)).astype(F32)
        ct_ref[p] = jnp.cos(angle)
        ct_ref[moms + p] = jnp.sin(angle)


def main_kernel(n_pieces, n_fac, *refs):
    pieces, refs = refs[:n_pieces], refs[n_pieces:]
    facs, refs = refs[: 2 * n_fac], refs[2 * n_fac :]
    et_ref, ee_ref, ct_ref, per_ref, cor_ref, w_ref, t_ref, stage_ref, out_ref, sem = refs
    nb = facs[0].shape[0]
    half = facs[0].shape[1] // 2
    spins = len(SPIN_SIGNS)
    nd = pieces[0].shape[-1]
    nev = et_ref.shape[0] // 2
    sites = ct_ref.shape[1]
    colours = half // sites

    for i in range(2):
        f = sum(r[...].astype(F32) for r in facs[i::2])
        col = lax.broadcasted_iota(jnp.int32, f.shape, 1)
        w_r = jnp.where(col >= half, -f, f).astype(BF16)
        w_i = jnp.concatenate([f[:, half:], f[:, :half]], axis=1).astype(BF16)
        for k in range(2):
            at = (4 * i + 2 * k) * nb
            w_ref[at : at + nb, :] = w_r
            w_ref[at + nb : at + 2 * nb, :] = w_i

    for pair in range(spins // 2):
        cols = []
        for a in (2 * pair, 2 * pair + 1):
            rows = []
            for piece in pieces:
                for r in range(2):
                    rows.append(piece[r, a])
            cols.append(jnp.concatenate(rows, axis=0))
        right = jnp.concatenate(cols, axis=1)
        for r in range(2):
            for k0 in range(0, nev, 256):
                t = jnp.dot(et_ref[r * nev + k0 : r * nev + k0 + 256, :], right, preferred_element_type=F32)
                t_ref[r * nev + k0 : r * nev + k0 + 256, 2 * pair * nd : 2 * (pair + 1) * nd] = t.astype(BF16)
                for i in range(2):
                    a = 2 * pair + i
                    stage_ref[pl.ds((r * nev + k0) * spins + a, 256, stride=spins), :] = t[:, i * nd : (i + 1) * nd]
    out_ref[...] = stage_ref[...].astype(BF16)
    copy = pltpu.make_async_copy(out_ref, per_ref, sem)
    copy.start()

    lane = lax.broadcasted_iota(jnp.int32, (half, nd), 1)
    low_half = lane < 2 * nb
    low_quarter = lane % (2 * nb) < nb
    total = jnp.zeros((sites, 2 * sites), F32)
    for pair in range(spins // 2):
        s = jnp.dot(ee_ref[...], t_ref[:, 2 * pair * nd : 2 * (pair + 1) * nd], preferred_element_type=F32)
        for i in range(2):
            a = 2 * pair + i
            s_r, s_i = s[:half, i * nd : (i + 1) * nd], s[half:, i * nd : (i + 1) * nd]
            u = jnp.where(low_quarter, s_r, pltpu.roll(s_i, nb, 1))
            v = jnp.where(low_quarter, pltpu.roll(s_r, nd - nb, 1), s_i)
            lhs = []
            for z in (u, v):
                hi = z.astype(BF16).astype(F32)
                lo = z - hi
                lhs.append(jnp.where(low_half, hi, pltpu.roll(lo, 2 * nb, 1)))
                lhs.append(jnp.where(low_half, pltpu.roll(hi, nd - 2 * nb, 1), lo))
            for z in lhs:
                z = z.astype(BF16)
                q = jnp.dot(jnp.concatenate([z, z], axis=1), w_ref[...], preferred_element_type=F32)
                q = q * q
                q = sum(q[:, c : c + 2 * sites] for c in range(0, 2 * half, 2 * sites))
                q = sum(q[c : c + sites] for c in range(0, half, sites))
                total = total + q if SPIN_SIGNS[a] > 0 else total - q

    moms = ct_ref.shape[0] // 2
    row = lax.broadcasted_iota(jnp.int32, (2, moms), 0)
    col = lax.broadcasted_iota(jnp.int32, (2, moms), 1)
    cor = jnp.zeros((2, moms), F32)
    for i in range(2):
        for p in range(moms):
            value = jnp.sum(total * ct_ref[i * moms + p], axis=(0, 1), keepdims=True)
            cor = jnp.where((row == i) & (col == p), value, cor)
    cor_ref[...] = cor * (1.0 / (sites * nb))
    copy.wait()


def body(n_src, n_snk, solutions, eigvecs, momenta, ordering):
    _, n_times, _, spins, share, colours, nd = solutions.shape
    _, _, sites, _, nev = eigvecs.shape
    nb = nd // spins
    half = colours * sites
    me, src = lax.axis_index("snk"), lax.axis_index("src")
    sol = solutions[0].transpose(0, 1, 2, 4, 3, 5).reshape(n_times, 2, spins, colours * share, nd)
    eig = eigvecs[0].transpose(0, 2, 1, 3)

    pieces = [lax.dynamic_index_in_dim(sol, me ^ j, 0, keepdims=False) for j in range(n_snk)]
    for j in range(1, n_snk):
        pieces[j] = lax.ppermute(pieces[j], "snk", [(i, i ^ j) for i in range(n_snk)])

    fac = pl.pallas_call(
        factors_kernel,
        out_shape=[jax.ShapeDtypeStruct((nb, 2 * half), BF16)] * 2,
        in_specs=[VMEM, VMEM],
        out_specs=[VMEM, VMEM],
        compiler_params=params(8),
        name="factors",
    )(ordering[None, :], eig)
    fac = jnp.stack(fac)
    own = jnp.where(me == src, fac, jnp.zeros_like(fac))
    facs = [own]
    for j in range(1, n_snk):
        facs.append(lax.ppermute(fac, ("src", "snk"), [(s * n_snk + s, s * n_snk + (s ^ j)) for s in range(n_src)]))
    facs = [f[i] for f in facs for i in range(2)]

    aligned = share % 16 == 0
    if aligned:
        extra, extra_specs = [], []
        kernel = lambda counts, mom, e, *outs: prepare_kernel(counts, mom, e, None, *outs)
    else:
        place = jnp.argsort(me ^ jnp.arange(n_snk))
        whole = jnp.stack(pieces).reshape(n_snk, 2, spins, colours, share, nd)[place]
        pieces = [whole.transpose(1, 2, 3, 0, 4, 5).reshape(2, spins, half, nd)]
        extra, extra_specs = [eig.reshape(2, half, nev)], [VMEM]
        kernel = prepare_kernel
    et, ee, ct = pl.pallas_call(
        functools.partial(kernel, (n_snk, share)),
        out_shape=[
            jax.ShapeDtypeStruct((2 * nev, 2 * half), BF16),
            jax.ShapeDtypeStruct((2 * half, 2 * nev), BF16),
            jax.ShapeDtypeStruct((2 * momenta.shape[0], sites, 2 * sites), F32),
        ],
        in_specs=[SMEM, VMEM] + extra_specs,
        out_specs=[VMEM] * 3,
        compiler_params=params(16),
        name="prepare",
    )(momenta, eig, *extra)

    peramb, correlator = pl.pallas_call(
        functools.partial(main_kernel, len(pieces), len(facs) // 2),
        out_shape=[
            jax.ShapeDtypeStruct((2 * nev * spins, nd), BF16),
            jax.ShapeDtypeStruct((2, momenta.shape[0]), F32),
        ],
        in_specs=[VMEM] * (len(pieces) + len(facs) + 3),
        out_specs=[ANY, VMEM],
        scratch_shapes=[
            pltpu.VMEM((8 * nb, 2 * half), BF16),
            pltpu.VMEM((2 * nev, spins * nd), BF16),
            pltpu.VMEM((2 * nev * spins, nd), F32),
            pltpu.VMEM((2 * nev * spins, nd), BF16),
            pltpu.SemaphoreType.DMA,
        ],
        compiler_params=params(32),
        name="main",
    )(*pieces, *facs, et, ee, ct)
    return (peramb.reshape(1, 1, 2, nev, spins, nd), correlator[None, None])


def solution(mesh):
    return jax.shard_map(
        functools.partial(body, mesh.shape["src"], mesh.shape["snk"]),
        mesh=mesh,
        in_specs=(
            P(("grp", "src"), None, None, None, "snk", None, None),
            P(("grp", "snk"), None, None, None, None),
            P(),
            P(),
        ),
        out_specs=(
            P(("grp", "snk"), "src", None, None, None, None),
            P(("grp", "snk"), "src", None, None),
        ),
        check_vma=False,
    )
```
